32 devices in a mesh: dp: 4 (over z), expert: 8 (over y, x, core).
Axes of the slice: x: 2, y: 2, z: 4, core: 2. Of those that a mesh axis runs over, the one named last changes fastest.
Arguments:
- tokens: bfloat16 [1024, 4096], P('expert', 'dp'), may hold values from -6 to 6
- grad_out: bfloat16 [1024, 4096], P('expert', 'dp'), may hold values from -6 to 6
- expert_ids: int32 [1024, 2], P('expert'), may hold values from 0 to 7, all different within a row; in each aligned block of 128 rows (0 to 127, 128 to 255, ...) at most 48 rows name the same one
- route_weights: float32 [1024, 2], P('expert'), may hold values from 0.05 to 1
- gate_weight: bfloat16 [8, 4096, 768], P('expert', 'dp'), may hold values from -0.09375 to 0.09375
- up_weight: bfloat16 [8, 4096, 768], P('expert', 'dp'), may hold values from -0.09375 to 0.09375
- down_weight: bfloat16 [8, 768, 4096], P('expert', None, 'dp'), may hold values from -0.21875 to 0.21875
Outputs:
- mixed: bfloat16 [1024, 4096], P('expert', 'dp')
- grad_tokens: bfloat16 [1024, 4096], P('expert', 'dp')
- grad_route: float32 [1024, 2], P('expert')
- grad_gate: bfloat16 [8, 4096, 768], P('expert', 'dp')
- grad_up: bfloat16 [8, 4096, 768], P('expert', 'dp')
- grad_down: bfloat16 [8, 768, 4096], P('expert', None, 'dp')
The draws below stay inside these ranges and needn't reach their ends.
Inputs may be any that keep to these rules, and one draw needn't show every extreme that they name: `expert_ids`: each token names 2 different experts; in each aligned block of 128 tokens (the tokens held by each position along `expert`) no expert is named by more than 48 tokens, a bound that some block reaches.
All inputs are finite; a program needn't handle non-finite values.
Results may differ from the reference program's by a relative error of at most 0.029.
Values may be sent and summed in bfloat16 or wider, within the bound.
No kernel may reach another device: no remote copies, remote signals or barrier semaphores. Data moves between devices by JAX's collectives and lax.ppermute only.
A program may use at most 64 MiB of HBM per device.

```python
import math
import jax
import jax.numpy as jnp
import numpy as np
from jax import lax

D = 4096
H = 768
TOK_DEV = 128
EXPERTS = 8
TOP = 2
CAP = 48
TOKENS = 1024
N_DP = 4
N_EXPERT = 8


def block_levels(own_key, extent, split, low, largest):
    loudness, own = 1.0, jax.random.fold_in(own_key, 6)
    for dim, shards_of in split:
        steps = jnp.exp(jax.random.uniform(jax.random.fold_in(own, dim), (shards_of,), jnp.float32, low / len(split), largest / len(split)))
        loudness = loudness * jnp.repeat(steps, extent[dim] // shards_of).reshape([-1 if axis == dim else 1 for axis in range(len(extent))])
    return loudness


def deal_out(stream_key, own, number, rows, number_of, top, most, slope):
    order = jax.random.permutation(stream_key, number_of)
    packed, usual = portions_of(number_of, rows * top, most, slope, True), portions_of(number_of, rows * top, most, slope, False)
    places = jnp.arange(number_of)

    def named(lengths, offset_by):
        used = int((lengths > 0).sum())
        fixed = max(1, used // 4)
        shifted = fixed + (places - fixed + offset_by * (used - fixed)) % max(1, number_of - fixed)
        return jnp.zeros((number_of,), jnp.int32).at[order[jnp.where(places < fixed, places, shifted)]].set(jnp.asarray(lengths, jnp.int32))

    lengths = jnp.where(number % 4 == 0, named(packed, number // 4), named(usual, number - number // 4 - 1))
    mixed = jax.random.permutation(jax.random.fold_in(own, 3), number_of)
    source_of, receiver = mixed[0:number_of // 2 * 2:2], mixed[1:number_of // 2 * 2:2]
    room = jnp.minimum(lengths[source_of] - 1, most - lengths[receiver]) // 2
    room = jnp.where((source_of == order[0]) | (receiver == order[0]) | (lengths[receiver] == 0), 0, jnp.maximum(room, 0))
    shifted = jax.random.randint(jax.random.fold_in(own, 4), (number_of // 2,), 0, 1 << 20) % (room + 1)
    lengths = lengths.at[source_of].add(-shifted).at[receiver].add(shifted)
    labels = jnp.searchsorted(jnp.cumsum(lengths), jnp.arange(rows * top), side="right").astype(jnp.int32)
    listing = labels.reshape(top, rows).T
    listing = listing[jax.random.permutation(jax.random.fold_in(own, 1), rows)]
    offset_by = jax.random.randint(jax.random.fold_in(own, 2), (rows, 1), 0, top)
    return jnp.take_along_axis(listing, (jnp.arange(top)[None, :] + offset_by) % top, axis=1)


def portions_of(count, total, limit, skew, full):
    weights = [(1 << 20) // math.isqrt(standing ** skew) + 1 for standing in range(1, count + 1)]
    largest = limit if full else min(limit, max(-(-total // count), total * weights[0] // sum(weights)))
    least = 1 if total - largest >= count - 1 else 0
    holding, rest = [largest] + [least] * (count - 1), total - largest - least * (count - 1)
    while rest > 0:
        free = [i for i in range(1, count) if holding[i] < largest] or [i for i in range(1, count) if holding[i] < limit]
        pool, left = sum([weights[i] for i in free]), rest
        for i in free:
            extra = min(limit - holding[i], max(1, left * weights[i] // pool), rest)
            holding[i] = holding[i] + extra
            rest = rest - extra
    return np.array(holding)


def gaussian(own_key, shape, scale, reach, pieces=(), kind=jnp.bfloat16):
    entries = jax.random.normal(own_key, shape, jnp.float32) * scale
    if len(pieces) > 0:
        entries = block_levels(own_key, shape, pieces, -0.22, 0.18) * entries
    return jnp.clip(entries, min=-reach, max=reach).astype(kind)


def setup_inputs(seed: int = 0) -> dict:
    key_list = jax.random.split(jax.random.key(seed), 8)
    tokens = gaussian(key_list[0], (TOKENS, D), 1.0, 6.0, ((0, 8), (1, 4)))
    grad_out = gaussian(key_list[1], (TOKENS, D), 1.0, 6.0, ((0, 8), (1, 4)))
    expert_ids_keys = jax.random.split(jax.random.fold_in(key_list[2], 1), TOKENS // TOK_DEV)
    expert_ids_turns = jax.random.permutation(jax.random.fold_in(key_list[2], 3), TOKENS // TOK_DEV)
    expert_ids = jax.vmap(lambda own, number: deal_out(jax.random.fold_in(key_list[2], 2), own, number, TOK_DEV, EXPERTS, TOP, CAP, 2))(expert_ids_keys, expert_ids_turns).reshape((TOKENS, TOP))
    route_weights = jnp.clip(jnp.exp(math.log(1.0) - 2.9957323 * jax.random.uniform(key_list[3], (TOKENS, TOP), jnp.float32) ** block_levels(key_list[3], (TOKENS, TOP), ((0, 8),), -0.2, 0.2)), 0.05, 1.0)
    gate_weight = gaussian(key_list[4], (EXPERTS, D, H), D ** -0.5, 0.09375, ((0, 8), (1, 4)))
    up_weight = gaussian(key_list[5], (EXPERTS, D, H), D ** -0.5, 0.09375, ((0, 8), (1, 4)))
    down_weight = gaussian(key_list[6], (EXPERTS, H, D), H ** -0.5, 0.21875, ((0, 8), (2, 4)))
    return {"tokens": tokens, "grad_out": grad_out, "expert_ids": expert_ids, "route_weights": route_weights, "gate_weight": gate_weight, "up_weight": up_weight, "down_weight": down_weight}


def block_partial(first_operand, second_operand, pattern):
    partial_value = jnp.einsum(pattern, first_operand.astype(jnp.float32), second_operand.astype(jnp.float32))
    rounded = lax.optimization_barrier(partial_value.astype(jnp.bfloat16))
    return jnp.sum(rounded.astype(jnp.float32), axis=0)


def activate(gate_sum, up_sum, back_sum):
    gate_sigmoid = jax.nn.sigmoid(gate_sum)
    swished = gate_sum * gate_sigmoid
    hidden = (swished * up_sum).astype(jnp.bfloat16)
    gate_grad = (back_sum * up_sum * gate_sigmoid * (1.0 + gate_sum * (1.0 - gate_sigmoid))).astype(jnp.bfloat16)
    up_grad = (back_sum * swished).astype(jnp.bfloat16)
    return hidden, gate_grad, up_grad


def reference(tokens, grad_out, expert_ids, route_weights, gate_weight, up_weight, down_weight):
    capacity = N_EXPERT * CAP
    feature_share = D // N_DP
    flat_ids = expert_ids.reshape(-1).astype(jnp.int32)
    assigned = flat_ids.shape[0]
    onehot = (flat_ids[:, None] == jnp.arange(EXPERTS, dtype=jnp.int32)[None, :]).astype(jnp.int32)
    before = jnp.cumsum(onehot, axis=0) - onehot
    position = jnp.sum(before * onehot, axis=1).astype(jnp.int32)
    slot_index = (flat_ids * capacity + position).astype(jnp.int32)
    owners = jnp.zeros((EXPERTS * capacity,), jnp.int32).at[slot_index].set(jnp.arange(assigned, dtype=jnp.int32) + 1)
    owners = owners.reshape(EXPERTS, capacity)
    flat_weights = route_weights.reshape(-1)

    def expert_pass(inputs):
        expert_owners, w_gate, w_up, w_down = inputs
        filled = expert_owners > 0
        source = jnp.maximum(expert_owners - 1, 0)
        token_index = source // TOP
        expert_rows = jnp.where(filled[:, None], tokens[token_index], jnp.zeros((), jnp.bfloat16))
        scaled = flat_weights[source][:, None] * grad_out[token_index].astype(jnp.float32)
        expert_grads = jnp.where(filled[:, None], scaled, jnp.zeros((), jnp.float32)).astype(jnp.bfloat16)
        row_blocks = expert_rows.reshape(capacity, N_DP, feature_share)
        grad_blocks = expert_grads.reshape(capacity, N_DP, feature_share)
        gate_sum = block_partial(row_blocks, w_gate.reshape(N_DP, feature_share, H), 'rbd,bdh->brh')
        up_sum = block_partial(row_blocks, w_up.reshape(N_DP, feature_share, H), 'rbd,bdh->brh')
        back_sum = block_partial(grad_blocks, w_down.reshape(H, N_DP, feature_share), 'rbd,hbd->brh')
        hidden, gate_grad, up_grad = activate(gate_sum, up_sum, back_sum)
        out_rows = jnp.dot(hidden, w_down, preferred_element_type=jnp.float32).astype(jnp.bfloat16)
        input_rows = (jnp.dot(gate_grad, w_gate.T, preferred_element_type=jnp.float32)
                      + jnp.dot(up_grad, w_up.T, preferred_element_type=jnp.float32)).astype(jnp.bfloat16)
        grad_gate_e = jnp.dot(expert_rows.T, gate_grad, preferred_element_type=jnp.float32).astype(jnp.bfloat16)
        grad_up_e = jnp.dot(expert_rows.T, up_grad, preferred_element_type=jnp.float32).astype(jnp.bfloat16)
        grad_down_e = jnp.dot(hidden.T, expert_grads, preferred_element_type=jnp.float32).astype(jnp.bfloat16)
        return out_rows, input_rows, grad_gate_e, grad_up_e, grad_down_e

    out_all, input_all, grad_gate, grad_up, grad_down = lax.map(expert_pass, (owners, gate_weight, up_weight, down_weight))
    out_assign = out_all.reshape(EXPERTS * capacity, D)[slot_index].reshape(TOKENS, TOP, D)
    input_assign = input_all.reshape(EXPERTS * capacity, D)[slot_index].reshape(TOKENS, TOP, D)
    mixed = jnp.zeros((TOKENS, D), jnp.float32)
    grad_tokens = jnp.zeros((TOKENS, D), jnp.float32)
    grad_columns = []
    grad_float = grad_out.astype(jnp.float32)
    for column in range(TOP):
        out_float = out_assign[:, column].astype(jnp.float32)
        mixed = mixed + route_weights[:, column][:, None] * out_float
        grad_tokens = grad_tokens + input_assign[:, column].astype(jnp.float32)
        grad_columns.append(jnp.sum(grad_float * out_float, axis=1))
    grad_route = jnp.stack(grad_columns, axis=1)
    return (mixed.astype(jnp.bfloat16), grad_tokens.astype(jnp.bfloat16), grad_route,
            grad_gate, grad_up, grad_down)
```

```python
import functools

import jax
import jax.numpy as jnp
from jax import lax
from jax.experimental import pallas as pl
from jax.experimental.pallas import tpu as pltpu
from jax.sharding import PartitionSpec as P


BF = jnp.bfloat16
F32 = jnp.float32
R_LANES = 128


def tile_of(size, most=256):
    return most if size % most == 0 else size


def dot(a, b, ca, cb):
    return lax.dot_general(a, b, (((ca,), (cb,)), ((), ())), preferred_element_type=F32)


def selection(ids_ref, me, rows, cap, tok):
    row = lax.broadcasted_iota(jnp.int32, (rows, 1), 0).astype(F32)
    offset = jnp.floor((row + 0.5) / cap)
    slot = row - offset * cap
    expert = offset.astype(jnp.int32) ^ me
    first = ids_ref[0:1, :] == expert
    second = ids_ref[1:2, :] == expert
    named = jnp.logical_or(first, second)
    earlier = (
        lax.broadcasted_iota(jnp.int32, (tok, tok), 0)
        < lax.broadcasted_iota(jnp.int32, (tok, tok), 1)
    )
    before = dot(jnp.where(named, 1.0, 0.0).astype(BF), jnp.where(earlier, 1.0, 0.0).astype(BF), 1, 0)
    chosen = jnp.logical_and(named, before == slot)
    return first, second, chosen


def send_kernel(cap, ids_ref, p_ref, tok_ref, grad_ref, *outs):
    me = lax.axis_index("expert")
    tok, width = tok_ref.shape
    rows = cap * len(outs)
    first, second, chosen = selection(ids_ref, me, rows, cap, tok)
    scale = jnp.where(jnp.logical_and(chosen, first), p_ref[0:1, :], 0.0)
    scale = scale + jnp.where(jnp.logical_and(chosen, second), p_ref[1:2, :], 0.0)
    scale = jnp.sum(scale, axis=1, keepdims=True)
    pick = jnp.where(chosen, 1.0, 0.0).astype(BF)
    x = dot(pick, tok_ref[...], 1, 0).astype(BF)
    g = (dot(pick, grad_ref[...], 1, 0) * scale).astype(BF)
    for i, out in enumerate(outs):
        out[:, :width] = x[i * cap : (i + 1) * cap]
        out[:, width:] = g[i * cap : (i + 1) * cap]


def whole(shape):
    return pl.BlockSpec(shape, lambda *_: (0,) * len(shape))


def send_rows(ids, p, tokens, grad, n, cap):
    width = tokens.shape[1]
    return pl.pallas_call(
        functools.partial(send_kernel, cap),
        out_shape=[jax.ShapeDtypeStruct((cap, 2 * width), BF)] * n,
        name="send_rows",
        cost_estimate=pl.CostEstimate(
            flops=4 * cap * n * tokens.size, bytes_accessed=8 * tokens.size, transcendentals=0
        ),
    )(ids, p, tokens, grad)


def gather_parts(refs, lo, hi):
    parts = [r[:, lo:hi] for r in refs]
    return parts[0] if len(parts) == 1 else jnp.concatenate(parts, axis=0)


def forward_kernel(count, *refs):
    parts, (wg, wu, wd, out) = refs[:count], refs[count:]
    width = wg.shape[0]
    x = gather_parts(parts, 0, width)
    g = gather_parts(parts, width, 2 * width)
    out[0] = dot(x, wg[...], 1, 0).astype(BF)
    out[1] = dot(x, wu[...], 1, 0).astype(BF)
    out[2] = dot(g, wd[...], 1, 1).astype(BF)


def forward(parts, wg, wu, wd):
    width, hidden = wg.shape
    rows = sum(p.shape[0] for p in parts)
    t = tile_of(hidden)
    return pl.pallas_call(
        functools.partial(forward_kernel, len(parts)),
        grid=(hidden // t,),
        in_specs=[whole(p.shape) for p in parts]
        + [
            pl.BlockSpec((width, t), lambda j: (0, j)),
            pl.BlockSpec((width, t), lambda j: (0, j)),
            pl.BlockSpec((t, width), lambda j: (j, 0)),
        ],
        out_specs=pl.BlockSpec((3, rows, t), lambda j: (0, 0, j)),
        out_shape=jax.ShapeDtypeStruct((3, rows, hidden), BF),
        name="forward_rows",
        cost_estimate=pl.CostEstimate(
            flops=6 * rows * width * hidden, bytes_accessed=6 * width * hidden, transcendentals=0
        ),
    )(*parts, wg, wu, wd)


def backward_kernel(count, is_end, s_ref, r_ref, wg, wu, wd, act, *outs):
    j = pl.program_id(0)
    t = wd.shape[1]
    cap = outs[0].shape[0]
    width = (outs[0].shape[1] - R_LANES) // 2

    @pl.when(j == 0)
    def _():
        total = s_ref[...]
        if is_end is not None:
            total = jnp.where(is_end(), r_ref[...], total)
        total = total.astype(F32)
        gate, up, back = total[0], total[1], total[2]
        sig = jax.nn.sigmoid(gate)
        swished = gate * sig
        hidden = (swished * up).astype(BF)
        act[0] = hidden
        act[1] = (back * up * sig * (1.0 + gate * (1.0 - sig))).astype(BF)
        act[2] = (back * swished).astype(BF)
        inner = jnp.sum(hidden.astype(F32) * back, axis=1, keepdims=True)
        high = inner.astype(BF)
        rest = inner - high.astype(F32)
        middle = rest.astype(BF)
        low = (rest - middle.astype(F32)).astype(BF)
        lane = lax.broadcasted_iota(jnp.int32, (inner.shape[0], R_LANES), 1)
        zero = jnp.zeros((), F32)
        pieces = jnp.where(lane == 0, high.astype(F32), zero)
        pieces = jnp.where(lane == 1, middle.astype(F32), pieces)
        pieces = jnp.where(lane == 2, low.astype(F32), pieces).astype(BF)
        for i, out in enumerate(outs):
            out[:, 2 * width :] = pieces[i * cap : (i + 1) * cap]

    o = dot(act[0], wd[...], 1, 0).astype(BF)
    dx = (dot(act[1], wg[...], 1, 1) + dot(act[2], wu[...], 1, 1)).astype(BF)
    left = pl.multiple_of(j * t, t)
    right = pl.multiple_of(width + j * t, t)
    for i, out in enumerate(outs):
        out[:, pl.ds(left, t)] = o[i * cap : (i + 1) * cap]
        out[:, pl.ds(right, t)] = dx[i * cap : (i + 1) * cap]


def backward(total, other, is_end, count, wg, wu, wd):
    width, hidden = wg.shape
    rows = total.shape[1]
    cap = rows // count
    t = tile_of(width)
    return pl.pallas_call(
        functools.partial(backward_kernel, count, is_end),
        grid=(width // t,),
        in_specs=[whole(total.shape), whole(other.shape)]
        + [
            pl.BlockSpec((t, hidden), lambda j: (j, 0)),
            pl.BlockSpec((t, hidden), lambda j: (j, 0)),
            pl.BlockSpec((hidden, t), lambda j: (0, j)),
        ],
        out_specs=[whole(total.shape)] + [whole((cap, 2 * width + R_LANES))] * count,
        out_shape=[jax.ShapeDtypeStruct(total.shape, BF)]
        + [jax.ShapeDtypeStruct((cap, 2 * width + R_LANES), BF)] * count,
        name="backward_rows",
        cost_estimate=pl.CostEstimate(
            flops=6 * rows * width * hidden, bytes_accessed=6 * width * hidden, transcendentals=rows * hidden
        ),
    )(total, other, wg, wu, wd)


def grads_kernel(nparts, nacts, *refs):
    xs, gs, acts = refs[:nparts], refs[nparts : 2 * nparts], refs[2 * nparts : 2 * nparts + nacts]
    dg, du, dd = refs[2 * nparts + nacts :]
    x = gather_parts(xs, 0, xs[0].shape[1])
    g = gather_parts(gs, 0, gs[0].shape[1])
    h, gg, ug = (
        acts[0][i] if nacts == 1 else jnp.concatenate([a[i] for a in acts], axis=0) for i in range(3)
    )
    dg[...] = dot(x, gg, 0, 0).astype(BF)
    du[...] = dot(x, ug, 0, 0).astype(BF)
    dd[...] = dot(h, g, 0, 0).astype(BF)


def weight_grads(parts, acts, width, hidden):
    t = tile_of(width)
    rows = sum(p.shape[0] for p in parts)
    steps = width // t
    return pl.pallas_call(
        functools.partial(grads_kernel, len(parts), len(acts)),
        grid=(steps,),
        in_specs=[pl.BlockSpec((p.shape[0], t), lambda j: (0, j)) for p in parts]
        + [pl.BlockSpec((p.shape[0], t), lambda j: (0, j + steps)) for p in parts]
        + [whole(a.shape) for a in acts],
        out_specs=[
            pl.BlockSpec((t, hidden), lambda j: (j, 0)),
            pl.BlockSpec((t, hidden), lambda j: (j, 0)),
            pl.BlockSpec((hidden, t), lambda j: (0, j)),
        ],
        out_shape=[
            jax.ShapeDtypeStruct((width, hidden), BF),
            jax.ShapeDtypeStruct((width, hidden), BF),
            jax.ShapeDtypeStruct((hidden, width), BF),
        ],
        name="weight_grads",
        cost_estimate=pl.CostEstimate(
            flops=6 * rows * width * hidden, bytes_accessed=6 * width * hidden, transcendentals=0
        ),
    )(*parts, *parts, *acts)


def merge_kernel(cap, width, count, *refs):
    ids_ref, p_ref = refs[:2]
    parts = refs[2 : 2 + count]
    mixed, grad_tok, route = refs[2 + count :]
    me = lax.axis_index("expert")
    tok = mixed.shape[0]
    rows = sum(r.shape[0] for r in parts)
    first, second, chosen = selection(ids_ref, me, rows, cap, tok)
    one = jnp.where(jnp.logical_and(chosen, first), 1.0, 0.0).astype(BF)
    two = jnp.where(jnp.logical_and(chosen, second), 1.0, 0.0).astype(BF)
    eye = lax.broadcasted_iota(jnp.int32, (tok, tok), 0) == lax.broadcasted_iota(jnp.int32, (tok, tok), 1)
    p_one = jnp.sum(jnp.where(eye, p_ref[0:1, :], 0.0), axis=1, keepdims=True)
    p_two = jnp.sum(jnp.where(eye, p_ref[1:2, :], 0.0), axis=1, keepdims=True)
    out = gather_parts(parts, 0, width)
    mixed[...] = (p_one * dot(one, out, 0, 0) + p_two * dot(two, out, 0, 0)).astype(BF)
    dx = gather_parts(parts, width, 2 * width)
    both = jnp.where(chosen, 1.0, 0.0).astype(BF)
    grad_tok[...] = dot(both, dx, 0, 0).astype(BF)
    inner = gather_parts(parts, 2 * width, 2 * width + R_LANES)
    route[0:1, :] = jnp.sum(dot(inner, one, 0, 0), axis=0, keepdims=True) / p_ref[0:1, :]
    route[1:2, :] = jnp.sum(dot(inner, two, 0, 0), axis=0, keepdims=True) / p_ref[1:2, :]


def merge(ids, p, parts, cap, tok, width):
    return pl.pallas_call(
        functools.partial(merge_kernel, cap, width, len(parts)),
        out_shape=[
            jax.ShapeDtypeStruct((tok, width), BF),
            jax.ShapeDtypeStruct((tok, width), BF),
            jax.ShapeDtypeStruct(p.shape, F32),
        ],
        name="merge_rows",
        cost_estimate=pl.CostEstimate(flops=10**8, bytes_accessed=2 * 10**6, transcendentals=0),
    )(ids, p, *parts)


def local(tokens, grad_out, expert_ids, route_weights, gate_weight, up_weight, down_weight):
    n = lax.axis_size("expert")
    n_dp = lax.axis_size("dp")
    assert gate_weight.shape[0] == 1
    wg, wu, wd = gate_weight[0], up_weight[0], down_weight[0]
    width, hidden = wg.shape
    tok = tokens.shape[0]
    top = expert_ids.shape[1]
    cap = max(2, 3 * tok * top // (2 * n))
    ids, p = expert_ids.T, route_weights.T

    def swap(array, x):
        return lax.ppermute(array, "expert", [(i, i ^ x) for i in range(n)]) if x else array

    half = n_dp // 2

    def is_end():
        z = lax.axis_index("dp")
        return jnp.logical_and(z != half - 1, z != half)

    def reduce_dp(part):
        if n_dp == 1:
            return part, part, None
        if n_dp != 4:
            total = lax.psum(part, "dp")
            return total, total, None
        pair = part + lax.ppermute(part, "dp", [(0, 1), (3, 2)])
        total = pair + lax.ppermute(pair, "dp", [(1, 2), (2, 1)])
        other = lax.ppermute(total, "dp", [(1, 0), (2, 3)])
        return total, other, is_end

    if n == 8:
        groups = [[0], [2, 3], [4, 5], [6, 7], [1]]
    else:
        groups = [list(range(n))]
    sends = send_rows(ids, p, tokens, grad_out, n, cap)
    order = [x for group in groups for x in group]
    arrived = {}
    if n == 8:
        for x in [2, 4, 3, 5, 6, 7, 1, 0]:
            arrived[x] = swap(sends[x], x)
        parts_of = [[arrived[x] for x in group] for group in groups]
    else:
        me = lax.axis_index("expert")
        stacked = jnp.stack(sends)[jnp.arange(n) ^ me]
        stacked = lax.all_to_all(stacked, "expert", split_axis=0, concat_axis=0, tiled=True)
        parts_of = [[stacked.reshape(n * cap, 2 * width)]]
    partials = [forward(parts, wg, wu, wd) for parts in parts_of]
    acts, back = [], {}
    for group, parts, partial in zip(groups, parts_of, partials):
        total, other, end = reduce_dp(partial)
        act, *outs = backward(total, other, end, len(parts), wg, wu, wd)
        acts.append(act)
        if n == 8:
            for x, out in zip(group, outs):
                back[x] = swap(out, x)
        else:
            rows = outs[0].reshape(n, cap, -1)
            rows = lax.all_to_all(rows, "expert", split_axis=0, concat_axis=0, tiled=True)
            rows = rows[jnp.arange(n) ^ me].reshape(n * cap, -1)
    returned = [back[x] for x in range(n)] if n == 8 else [rows]
    mixed, grad_tokens, route = merge(ids, p, returned, cap, tok, width)
    flat = [a for parts in parts_of for a in parts]
    dg, du, dd = weight_grads(flat, acts, width, hidden)
    return (mixed, grad_tokens, route.T, dg[None], du[None], dd[None])


def solution(mesh):
    placed = (
        P("expert", "dp"),
        P("expert", "dp"),
        P("expert", None),
        P("expert", None),
        P("expert", "dp", None),
        P("expert", "dp", None),
        P("expert", None, "dp"),
    )
    return jax.shard_map(
        local,
        mesh=mesh,
        in_specs=placed,
        out_specs=(
            P("expert", "dp"),
            P("expert", "dp"),
            P("expert", None),
            P("expert", "dp", None),
            P("expert", "dp", None),
            P("expert", None, "dp"),
        ),
        check_vma=False,
    )
```

```python
import functools

import jax
import jax.numpy as jnp
from jax import lax
from jax.experimental import pallas as pl
from jax.experimental.pallas import tpu as pltpu
from jax.sharding import PartitionSpec as P


BF = jnp.bfloat16
F32 = jnp.float32
R_LANES = 128
GRANT = 16 * 2**20


def tile_of(size, most=256):
    return most if size % most == 0 else size


def dot(a, b, ca, cb):
    return lax.dot_general(a, b, (((ca,), (cb,)), ((), ())), preferred_element_type=F32)


def selection(ids_ref, me, rows, cap, tok):
    row = lax.broadcasted_iota(jnp.int32, (rows, 1), 0).astype(F32)
    offset = jnp.floor((row + 0.5) / cap)
    slot = row - offset * cap
    expert = offset.astype(jnp.int32) ^ me
    first = ids_ref[0:1, :] == expert
    second = ids_ref[1:2, :] == expert
    named = jnp.logical_or(first, second)
    earlier = (
        lax.broadcasted_iota(jnp.int32, (tok, tok), 0)
        < lax.broadcasted_iota(jnp.int32, (tok, tok), 1)
    )
    before = dot(jnp.where(named, 1.0, 0.0).astype(BF), jnp.where(earlier, 1.0, 0.0).astype(BF), 1, 0)
    chosen = jnp.logical_and(named, before == slot)
    return first, second, chosen


def send_kernel(cap, n, ids_ref, p_ref, tok_ref, grad_ref, wg_ref, wu_ref, wd_ref, *rest):
    outs, (ids, p, wg, wu, wd), (tok, grad, sems) = rest[:n], rest[n : n + 5], rest[n + 5 :]
    pairs = [(ids_ref, ids), (p_ref, p), (tok_ref, tok), (grad_ref, grad), (wg_ref, wg), (wu_ref, wu), (wd_ref, wd)]
    copies = [pltpu.make_async_copy(a, b, sems.at[i]) for i, (a, b) in enumerate(pairs)]
    for copy in copies:
        copy.start()
    for copy in copies[:4]:
        copy.wait()
    me = lax.axis_index("expert")
    count, width = tok.shape
    rows = cap * n
    first, second, chosen = selection(ids, me, rows, cap, count)
    scale = jnp.where(jnp.logical_and(chosen, first), p[0:1, :], 0.0)
    scale = scale + jnp.where(jnp.logical_and(chosen, second), p[1:2, :], 0.0)
    scale = jnp.sum(scale, axis=1, keepdims=True)
    pick = jnp.where(chosen, 1.0, 0.0).astype(BF)
    x = dot(pick, tok[...], 1, 0).astype(BF)
    g = (dot(pick, grad[...], 1, 0) * scale).astype(BF)
    for i, out in enumerate(outs):
        out[:, :width] = x[i * cap : (i + 1) * cap]
        out[:, width:] = g[i * cap : (i + 1) * cap]
    for copy in copies[4:]:
        copy.wait()


def whole(shape):
    return pl.BlockSpec(shape, lambda *_: (0,) * len(shape))


HBM = pl.BlockSpec(memory_space=pltpu.HBM)
UNREAD = pl.BlockSpec(memory_space=pl.ANY)


def params(grant=GRANT):
    return pltpu.CompilerParams(vmem_limit_bytes=grant)


def send_rows(ids, p, tokens, grad, weights, n, cap):
    width = tokens.shape[1]
    keep = (ids, p, *weights)
    inputs = [pltpu.with_memory_space_constraint(a, pltpu.HBM) for a in (ids, p, tokens, grad, *weights)]
    return pl.pallas_call(
        functools.partial(send_kernel, cap, n),
        in_specs=[HBM] * 7,
        out_shape=[pltpu.VMEM((cap, 2 * width), BF)] * n + [pltpu.VMEM(a.shape, a.dtype) for a in keep],
        scratch_shapes=[
            pltpu.VMEM(tokens.shape, BF),
            pltpu.VMEM(grad.shape, BF),
            pltpu.SemaphoreType.DMA((7,)),
        ],
        name="send_rows",
        compiler_params=params(),
        cost_estimate=pl.CostEstimate(
            flops=4 * cap * n * tokens.size, bytes_accessed=8 * tokens.size, transcendentals=0
        ),
    )(*inputs)


def hold(arrays, after):
    return pl.pallas_call(
        lambda *_: None,
        in_specs=[UNREAD] * (len(arrays) + 1),
        out_specs=[UNREAD] * len(arrays),
        out_shape=[jax.ShapeDtypeStruct(a.shape, a.dtype) for a in arrays],
        input_output_aliases={i: i for i in range(len(arrays))},
        name="hold",
        compiler_params=params(),
    )(*arrays, after)


def add_kernel(a, b, _, out):
    out[...] = (a[...].astype(F32) + b[...].astype(F32)).astype(BF)


def add_rows(a, b, after):
    return pl.pallas_call(
        add_kernel,
        in_specs=[whole(a.shape), whole(b.shape), UNREAD],
        out_specs=whole(a.shape),
        out_shape=jax.ShapeDtypeStruct(a.shape, BF),
        name="add_rows",
        compiler_params=params(),
        cost_estimate=pl.CostEstimate(flops=a.size, bytes_accessed=6 * a.size, transcendentals=0),
    )(a, b, after)


def gather_parts(refs, lo, hi):
    parts = [r[:, lo:hi] for r in refs]
    return parts[0] if len(parts) == 1 else jnp.concatenate(parts, axis=0)


def forward_kernel(count, *refs):
    parts, (wg, wu, wd, _, out) = refs[:count], refs[count:]
    width = wg.shape[0]
    x = gather_parts(parts, 0, width)
    g = gather_parts(parts, width, 2 * width)
    out[0] = dot(x, wg[...], 1, 0).astype(BF)
    out[1] = dot(x, wu[...], 1, 0).astype(BF)
    out[2] = dot(g, wd[...], 1, 1).astype(BF)


def forward(parts, weights, after):
    wg, wu, wd = weights
    width, hidden = wg.shape
    rows = sum(p.shape[0] for p in parts)
    t = hidden
    return pl.pallas_call(
        functools.partial(forward_kernel, len(parts)),
        grid=(hidden // t,),
        in_specs=[whole(p.shape) for p in parts]
        + [
            pl.BlockSpec((width, t), lambda j: (0, j)),
            pl.BlockSpec((width, t), lambda j: (0, j)),
            pl.BlockSpec((t, width), lambda j: (j, 0)),
            UNREAD,
        ],
        out_specs=pl.BlockSpec((3, rows, t), lambda j: (0, 0, j)),
        out_shape=jax.ShapeDtypeStruct((3, rows, hidden), BF),
        name="forward_rows",
        compiler_params=params(),
        cost_estimate=pl.CostEstimate(
            flops=6 * rows * width * hidden, bytes_accessed=6 * width * hidden, transcendentals=0
        ),
    )(*parts, wg, wu, wd, after)


def backward_kernel(skip, is_end, s_ref, r_ref, wg, wu, wd, *rest):
    act, *outs = rest[skip:]
    j = pl.program_id(0)
    t = wd.shape[1]
    cap = outs[0].shape[0]
    width = (outs[0].shape[1] - R_LANES) // 2

    @pl.when(j == 0)
    def _():
        total = s_ref[...]
        if is_end is not None:
            total = jnp.where(is_end(), r_ref[...], total)
        total = total.astype(F32)
        gate, up, back = total[0], total[1], total[2]
        sig = jax.nn.sigmoid(gate)
        swished = gate * sig
        hidden = (swished * up).astype(BF)
        act[0] = hidden
        act[1] = (back * up * sig * (1.0 + gate * (1.0 - sig))).astype(BF)
        act[2] = (back * swished).astype(BF)
        inner = jnp.sum(hidden.astype(F32) * back, axis=1, keepdims=True)
        high = inner.astype(BF)
        rest = inner - high.astype(F32)
        middle = rest.astype(BF)
        low = (rest - middle.astype(F32)).astype(BF)
        lane = lax.broadcasted_iota(jnp.int32, (inner.shape[0], R_LANES), 1)
        zero = jnp.zeros((), F32)
        pieces = jnp.where(lane == 0, high.astype(F32), zero)
        pieces = jnp.where(lane == 1, middle.astype(F32), pieces)
        pieces = jnp.where(lane == 2, low.astype(F32), pieces).astype(BF)
        for i, out in enumerate(outs):
            out[:, 2 * width :] = pieces[i * cap : (i + 1) * cap]

    o = dot(act[0], wd[...], 1, 0).astype(BF)
    dx = (dot(act[1], wg[...], 1, 1) + dot(act[2], wu[...], 1, 1)).astype(BF)
    left = pl.multiple_of(j * t, t)
    right = pl.multiple_of(width + j * t, t)
    for i, out in enumerate(outs):
        out[:, pl.ds(left, t)] = o[i * cap : (i + 1) * cap]
        out[:, pl.ds(right, t)] = dx[i * cap : (i + 1) * cap]


def backward(total, other, is_end, count, weights, after):
    wg, wu, wd = weights
    width, hidden = wg.shape
    rows = total.shape[1]
    cap = rows // count
    t = width
    return pl.pallas_call(
        functools.partial(backward_kernel, len(after), is_end),
        grid=(width // t,),
        in_specs=[whole(total.shape), whole(other.shape)]
        + [
            pl.BlockSpec((t, hidden), lambda j: (j, 0)),
            pl.BlockSpec((t, hidden), lambda j: (j, 0)),
            pl.BlockSpec((hidden, t), lambda j: (0, j)),
        ]
        + [UNREAD] * len(after),
        out_specs=[whole(total.shape)] + [whole((cap, 2 * width + R_LANES))] * count,
        out_shape=[jax.ShapeDtypeStruct(total.shape, BF)]
        + [jax.ShapeDtypeStruct((cap, 2 * width + R_LANES), BF)] * count,
        name="backward_rows",
        compiler_params=params(),
        cost_estimate=pl.CostEstimate(
            flops=6 * rows * width * hidden, bytes_accessed=6 * width * hidden, transcendentals=rows * hidden
        ),
    )(total, other, wg, wu, wd, *after)


def grads_kernel(nparts, nacts, *refs):
    xs, gs, acts = refs[:nparts], refs[nparts : 2 * nparts], refs[2 * nparts : 2 * nparts + nacts]
    dg, du, dd = refs[2 * nparts + nacts + 1 :]
    x = gather_parts(xs, 0, xs[0].shape[1])
    g = gather_parts(gs, 0, gs[0].shape[1])
    h, gg, ug = (
        acts[0][i] if nacts == 1 else jnp.concatenate([a[i] for a in acts], axis=0) for i in range(3)
    )
    dg[...] = dot(x, gg, 0, 0).astype(BF)
    du[...] = dot(x, ug, 0, 0).astype(BF)
    dd[...] = dot(h, g, 0, 0).astype(BF)


def weight_grads(parts, acts, width, hidden, after):
    t = tile_of(width)
    rows = sum(p.shape[0] for p in parts)
    steps = width // t
    return pl.pallas_call(
        functools.partial(grads_kernel, len(parts), len(acts)),
        grid=(steps,),
        in_specs=[pl.BlockSpec((p.shape[0], t), lambda j: (0, j)) for p in parts]
        + [pl.BlockSpec((p.shape[0], t), lambda j: (0, j + steps)) for p in parts]
        + [whole(a.shape) for a in acts]
        + [UNREAD],
        out_specs=[
            pl.BlockSpec((t, hidden), lambda j: (j, 0)),
            pl.BlockSpec((t, hidden), lambda j: (j, 0)),
            pl.BlockSpec((hidden, t), lambda j: (0, j)),
        ],
        out_shape=[
            jax.ShapeDtypeStruct((width, hidden), BF),
            jax.ShapeDtypeStruct((width, hidden), BF),
            jax.ShapeDtypeStruct((hidden, width), BF),
        ],
        name="weight_grads",
        compiler_params=params(),
        cost_estimate=pl.CostEstimate(
            flops=6 * rows * width * hidden, bytes_accessed=6 * width * hidden, transcendentals=0
        ),
    )(*parts, *parts, *acts, after)


def merge_kernel(cap, width, count, *refs):
    ids_ref, p_ref = refs[:2]
    parts = refs[2 : 2 + count]
    mixed, grad_tok, route = refs[3 + count :]
    me = lax.axis_index("expert")
    tok = mixed.shape[0]
    rows = sum(r.shape[0] for r in parts)
    first, second, chosen = selection(ids_ref, me, rows, cap, tok)
    one = jnp.where(jnp.logical_and(chosen, first), 1.0, 0.0).astype(BF)
    two = jnp.where(jnp.logical_and(chosen, second), 1.0, 0.0).astype(BF)
    eye = lax.broadcasted_iota(jnp.int32, (tok, tok), 0) == lax.broadcasted_iota(jnp.int32, (tok, tok), 1)
    p_one = jnp.sum(jnp.where(eye, p_ref[0:1, :], 0.0), axis=1, keepdims=True)
    p_two = jnp.sum(jnp.where(eye, p_ref[1:2, :], 0.0), axis=1, keepdims=True)
    out = gather_parts(parts, 0, width)
    mixed[...] = (p_one * dot(one, out, 0, 0) + p_two * dot(two, out, 0, 0)).astype(BF)
    dx = gather_parts(parts, width, 2 * width)
    both = jnp.where(chosen, 1.0, 0.0).astype(BF)
    grad_tok[...] = dot(both, dx, 0, 0).astype(BF)
    inner = gather_parts(parts, 2 * width, 2 * width + R_LANES)
    route[0:1, :] = jnp.sum(dot(inner, one, 0, 0), axis=0, keepdims=True) / p_ref[0:1, :]
    route[1:2, :] = jnp.sum(dot(inner, two, 0, 0), axis=0, keepdims=True) / p_ref[1:2, :]


def merge(ids, p, parts, cap, tok, width, after):
    return pl.pallas_call(
        functools.partial(merge_kernel, cap, width, len(parts)),
        in_specs=[whole(a.shape) for a in (ids, p, *parts)] + [UNREAD],
        out_shape=[
            jax.ShapeDtypeStruct((tok, width), BF),
            jax.ShapeDtypeStruct((tok, width), BF),
            jax.ShapeDtypeStruct(p.shape, F32),
        ],
        name="merge_rows",
        compiler_params=params(),
        cost_estimate=pl.CostEstimate(flops=10**8, bytes_accessed=2 * 10**6, transcendentals=0),
    )(ids, p, *parts, after)


def local(tokens, grad_out, expert_ids, route_weights, gate_weight, up_weight, down_weight):
    n = lax.axis_size("expert")
    n_dp = lax.axis_size("dp")
    assert gate_weight.shape[0] == 1
    weights = gate_weight[0], up_weight[0], down_weight[0]
    width, hidden = weights[0].shape
    tok = tokens.shape[0]
    top = expert_ids.shape[1]
    cap = max(2, 3 * tok * top // (2 * n))
    *sends, ids, p, wg, wu, wd = send_rows(expert_ids.T, route_weights.T, tokens, grad_out, weights, n, cap)
    weights = wg, wu, wd
    plan = chained if chainable(n, n_dp) else plain
    parts, acts, returned, last = plan(sends, weights, cap)
    dg, du, dd = weight_grads(parts, acts, width, hidden, last)
    mixed, grad_tokens, route = merge(ids, p, returned, cap, tok, width, last)
    return (mixed, grad_tokens, route.T, dg[None], du[None], dd[None])


def chainable(n, n_dp):
    return n == 8 and n_dp == 4


def plain(sends, weights, cap):
    n = len(sends)
    order = jnp.arange(n) ^ lax.axis_index("expert")
    rows = jnp.stack(sends)[order]
    rows = lax.all_to_all(rows, "expert", split_axis=0, concat_axis=0, tiled=True)
    rows = rows.reshape(n * cap, -1)
    total = lax.psum(forward([rows], weights, rows), "dp")
    act, out = backward(total, total, None, 1, weights, (rows,))
    back = lax.all_to_all(out.reshape(n, cap, -1), "expert", split_axis=0, concat_axis=0, tiled=True)
    return [rows], [act], [back[order].reshape(n * cap, -1)], act


CHUNKS = {"O": (0, 1), "P": (2, 4), "D": (6, 7), "Q": (3, 5)}
SCRIPT = (
    ("send", "O"),
    ("send", "P"),
    ("fwd", "O"),
    ("fwd", "P"),
    ("send", "D"),
    ("one", "O"),
    ("send", "Q"),
    ("fwd", "D"),
    ("one", "P"),
    ("two", "O"),
    ("fwd", "Q"),
    ("one", "D"),
    ("two", "P"),
    ("bwd", "O"),
    ("one", "Q"),
    ("two", "D"),
    ("bwd", "P"),
    ("two", "Q"),
    ("bwd", "D"),
    ("bwd", "Q", "O"),
)


def chained(sends, weights, cap):
    n = len(sends)
    half = lax.axis_size("dp") // 2

    def is_end():
        z = lax.axis_index("dp")
        return jnp.logical_and(z != half - 1, z != half)

    def swap(array, x):
        return lax.ppermute(array, "expert", [(i, i ^ x) for i in range(n)]) if x else array

    def along(array, op):
        pairs = {"fwd": [(0, 1), (3, 2)], "one": [(1, 2), (2, 1)], "two": [(1, 0), (2, 3)]}[op]
        return array, lax.ppermute(array, "dp", pairs)

    last = sends[0]
    rows, flow, acts, back = {0: sends[0]}, {}, {}, {}
    for op, name, *behind in SCRIPT:
        chunk = CHUNKS[name]
        if op == "send":
            fresh = [sends[x] for x in chunk]
            if last is not sends[0]:
                fresh = hold(fresh, last)
                last = fresh[0]
            for x, array in zip(chunk, fresh):
                rows[x] = swap(array, x)
            continue
        if op == "fwd":
            last = forward([rows[x] for x in chunk], weights, last)
        elif op in ("one", "two"):
            last = add_rows(*flow[name], last)
        else:
            after = [back[x] for other in behind for x in CHUNKS[other]]
            last, *outs = backward(*flow[name], is_end, len(chunk), weights, (last, *after))
        if op == "bwd":
            acts[name] = last
            for x, out in zip(chunk, outs):
                back[x] = swap(out, x)
        else:
            flow[name] = along(last, op)
    parts = [rows[x] for chunk in CHUNKS.values() for x in chunk]
    return parts, [acts[name] for name in CHUNKS], [back[x] for x in range(n)], last


def solution(mesh):
    placed = (
        P("expert", "dp"),
        P("expert", "dp"),
        P("expert", None),
        P("expert", None),
        P("expert", "dp", None),
        P("expert", "dp", None),
        P("expert", None, "dp"),
    )
    return jax.shard_map(
        local,
        mesh=mesh,
        in_specs=placed,
        out_specs=(
            P("expert", "dp"),
            P("expert", "dp"),
            P("expert", None),
            P("expert", "dp", None),
            P("expert", "dp", None),
            P("expert", None, "dp"),
        ),
        check_vma=False,
    )
```

```python
import functools

import jax
import jax.numpy as jnp
from jax import lax
from jax.experimental import pallas as pl
from jax.experimental.pallas import tpu as pltpu
from jax.sharding import PartitionSpec as P


BF = jnp.bfloat16
F32 = jnp.float32
R_LANES = 128
GRANT = 16 * 2**20


def tile_of(size, most=256):
    return most if size % most == 0 else size


def dot(a, b, ca, cb):
    return lax.dot_general(a, b, (((ca,), (cb,)), ((), ())), preferred_element_type=F32)


def selection(ids_ref, me, rows, cap, tok):
    row = lax.broadcasted_iota(jnp.int32, (rows, 1), 0).astype(F32)
    offset = jnp.floor((row + 0.5) / cap)
    slot = row - offset * cap
    expert = offset.astype(jnp.int32) ^ me
    first = ids_ref[0:1, :] == expert
    second = ids_ref[1:2, :] == expert
    named = jnp.logical_or(first, second)
    earlier = (
        lax.broadcasted_iota(jnp.int32, (tok, tok), 0)
        < lax.broadcasted_iota(jnp.int32, (tok, tok), 1)
    )
    before = dot(jnp.where(named, 1.0, 0.0).astype(BF), jnp.where(earlier, 1.0, 0.0).astype(BF), 1, 0)
    chosen = jnp.logical_and(named, before == slot)
    return first, second, chosen


def send_kernel(cap, n, ids_ref, p_ref, tok_ref, grad_ref, wg_ref, wu_ref, wd_ref, *rest):
    outs, (ids, p, wg, wu, wd) = rest[:n], rest[n : n + 5]
    one, two, tok, grad, sems = rest[n + 5 :]
    pairs = [(ids_ref, ids), (p_ref, p), (tok_ref, tok), (grad_ref, grad), (wg_ref, wg), (wu_ref, wu), (wd_ref, wd)]
    copies = [pltpu.make_async_copy(a, b, sems.at[i]) for i, (a, b) in enumerate(pairs)]
    for copy in copies:
        copy.start()
    for copy in copies[:4]:
        copy.wait()
    me = lax.axis_index("expert")
    count, width = tok.shape
    rows = cap * n
    first, second, chosen = selection(ids, me, rows, cap, count)
    scale = jnp.where(jnp.logical_and(chosen, first), p[0:1, :], 0.0)
    scale = scale + jnp.where(jnp.logical_and(chosen, second), p[1:2, :], 0.0)
    scale = jnp.sum(scale, axis=1, keepdims=True)
    one[...] = jnp.where(jnp.logical_and(chosen, first), 1.0, 0.0).astype(BF)
    two[...] = jnp.where(jnp.logical_and(chosen, second), 1.0, 0.0).astype(BF)
    pick = jnp.where(chosen, 1.0, 0.0).astype(BF)
    x = dot(pick, tok[...], 1, 0).astype(BF)
    g = (dot(pick, grad[...], 1, 0) * scale).astype(BF)
    for i, out in enumerate(outs):
        out[:, :width] = x[i * cap : (i + 1) * cap]
        out[:, width:] = g[i * cap : (i + 1) * cap]
    for copy in copies[4:]:
        copy.wait()


def whole(shape):
    return pl.BlockSpec(shape, lambda *_: (0,) * len(shape))


HBM = pl.BlockSpec(memory_space=pltpu.HBM)
UNREAD = pl.BlockSpec(memory_space=pl.ANY)


def params(grant=GRANT):
    return pltpu.CompilerParams(vmem_limit_bytes=grant)


def send_rows(ids, p, tokens, grad, weights, n, cap):
    width = tokens.shape[1]
    keep = (ids, p, *weights)
    inputs = [pltpu.with_memory_space_constraint(a, pltpu.HBM) for a in (ids, p, tokens, grad, *weights)]
    return pl.pallas_call(
        functools.partial(send_kernel, cap, n),
        in_specs=[HBM] * 7,
        out_shape=[pltpu.VMEM((cap, 2 * width), BF)] * n + [pltpu.VMEM(a.shape, a.dtype) for a in keep]
        + [pltpu.VMEM((cap * n, tokens.shape[0]), BF)] * 2,
        scratch_shapes=[
            pltpu.VMEM(tokens.shape, BF),
            pltpu.VMEM(grad.shape, BF),
            pltpu.SemaphoreType.DMA((7,)),
        ],
        name="send_rows",
        compiler_params=params(),
        cost_estimate=pl.CostEstimate(
            flops=4 * cap * n * tokens.size, bytes_accessed=8 * tokens.size, transcendentals=0
        ),
    )(*inputs)


def hold(arrays, after):
    return pl.pallas_call(
        lambda *_: None,
        in_specs=[UNREAD] * (len(arrays) + 1),
        out_specs=[UNREAD] * len(arrays),
        out_shape=[jax.ShapeDtypeStruct(a.shape, a.dtype) for a in arrays],
        input_output_aliases={i: i for i in range(len(arrays))},
        name="hold",
        compiler_params=params(),
    )(*arrays, after)


def add_kernel(a, b, _, out):
    out[...] = (a[...].astype(F32) + b[...].astype(F32)).astype(BF)


def add_rows(a, b, after):
    return pl.pallas_call(
        add_kernel,
        in_specs=[whole(a.shape), whole(b.shape), UNREAD],
        out_specs=whole(a.shape),
        out_shape=jax.ShapeDtypeStruct(a.shape, BF),
        name="add_rows",
        compiler_params=params(),
        cost_estimate=pl.CostEstimate(flops=a.size, bytes_accessed=6 * a.size, transcendentals=0),
    )(a, b, after)


def gather_parts(refs, lo, hi):
    parts = [r[:, lo:hi] for r in refs]
    return parts[0] if len(parts) == 1 else jnp.concatenate(parts, axis=0)


def forward_kernel(count, *refs):
    parts, (wg, wu, wd, _, out) = refs[:count], refs[count:]
    width = wg.shape[0]
    x = gather_parts(parts, 0, width)
    g = gather_parts(parts, width, 2 * width)
    out[0] = dot(x, wg[...], 1, 0).astype(BF)
    out[1] = dot(x, wu[...], 1, 0).astype(BF)
    out[2] = dot(g, wd[...], 1, 1).astype(BF)


def forward(parts, weights, after):
    wg, wu, wd = weights
    width, hidden = wg.shape
    rows = sum(p.shape[0] for p in parts)
    t = hidden
    return pl.pallas_call(
        functools.partial(forward_kernel, len(parts)),
        grid=(hidden // t,),
        in_specs=[whole(p.shape) for p in parts]
        + [
            pl.BlockSpec((width, t), lambda j: (0, j)),
            pl.BlockSpec((width, t), lambda j: (0, j)),
            pl.BlockSpec((t, width), lambda j: (j, 0)),
            UNREAD,
        ],
        out_specs=pl.BlockSpec((3, rows, t), lambda j: (0, 0, j)),
        out_shape=jax.ShapeDtypeStruct((3, rows, hidden), BF),
        name="forward_rows",
        compiler_params=params(),
        cost_estimate=pl.CostEstimate(
            flops=6 * rows * width * hidden, bytes_accessed=6 * width * hidden, transcendentals=0
        ),
    )(*parts, wg, wu, wd, after)


def backward_kernel(skip, is_end, s_ref, r_ref, wg, wu, wd, *rest):
    act, *outs = rest[skip:]
    j = pl.program_id(0)
    t = wd.shape[1]
    cap = outs[0].shape[0]
    width = (outs[0].shape[1] - R_LANES) // 2

    @pl.when(j == 0)
    def _():
        total = s_ref[...]
        if is_end is not None:
            total = jnp.where(is_end(), r_ref[...], total)
        total = total.astype(F32)
        gate, up, back = total[0], total[1], total[2]
        sig = jax.nn.sigmoid(gate)
        swished = gate * sig
        hidden = (swished * up).astype(BF)
        act[0] = hidden
        act[1] = (back * up * sig * (1.0 + gate * (1.0 - sig))).astype(BF)
        act[2] = (back * swished).astype(BF)
        inner = jnp.sum(hidden.astype(F32) * back, axis=1, keepdims=True)
        high = inner.astype(BF)
        rest = inner - high.astype(F32)
        middle = rest.astype(BF)
        low = (rest - middle.astype(F32)).astype(BF)
        lane = lax.broadcasted_iota(jnp.int32, (inner.shape[0], R_LANES), 1)
        zero = jnp.zeros((), F32)
        pieces = jnp.where(lane == 0, high.astype(F32), zero)
        pieces = jnp.where(lane == 1, middle.astype(F32), pieces)
        pieces = jnp.where(lane == 2, low.astype(F32), pieces).astype(BF)
        for i, out in enumerate(outs):
            out[:, 2 * width :] = pieces[i * cap : (i + 1) * cap]

    o = dot(act[0], wd[...], 1, 0).astype(BF)
    dx = (dot(act[1], wg[...], 1, 1) + dot(act[2], wu[...], 1, 1)).astype(BF)
    left = pl.multiple_of(j * t, t)
    right = pl.multiple_of(width + j * t, t)
    for i, out in enumerate(outs):
        out[:, pl.ds(left, t)] = o[i * cap : (i + 1) * cap]
        out[:, pl.ds(right, t)] = dx[i * cap : (i + 1) * cap]


def backward(total, other, is_end, count, weights, after):
    wg, wu, wd = weights
    width, hidden = wg.shape
    rows = total.shape[1]
    cap = rows // count
    t = width
    return pl.pallas_call(
        functools.partial(backward_kernel, len(after), is_end),
        grid=(width // t,),
        in_specs=[whole(total.shape), whole(other.shape)]
        + [
            pl.BlockSpec((t, hidden), lambda j: (j, 0)),
            pl.BlockSpec((t, hidden), lambda j: (j, 0)),
            pl.BlockSpec((hidden, t), lambda j: (0, j)),
        ]
        + [UNREAD] * len(after),
        out_specs=[whole(total.shape)] + [whole((cap, 2 * width + R_LANES))] * count,
        out_shape=[jax.ShapeDtypeStruct(total.shape, BF)]
        + [jax.ShapeDtypeStruct((cap, 2 * width + R_LANES), BF)] * count,
        name="backward_rows",
        compiler_params=params(),
        cost_estimate=pl.CostEstimate(
            flops=6 * rows * width * hidden, bytes_accessed=6 * width * hidden, transcendentals=rows * hidden
        ),
    )(total, other, wg, wu, wd, *after)


def grads_kernel(nparts, nacts, *refs):
    xs, gs, acts = refs[:nparts], refs[nparts : 2 * nparts], refs[2 * nparts : 2 * nparts + nacts]
    dg, du, dd = refs[2 * nparts + nacts + 1 :]
    x = gather_parts(xs, 0, xs[0].shape[1])
    g = gather_parts(gs, 0, gs[0].shape[1])
    h, gg, ug = (
        acts[0][i] if nacts == 1 else jnp.concatenate([a[i] for a in acts], axis=0) for i in range(3)
    )
    dg[...] = dot(x, gg, 0, 0).astype(BF)
    du[...] = dot(x, ug, 0, 0).astype(BF)
    dd[...] = dot(h, g, 0, 0).astype(BF)


def weight_grads(parts, acts, width, hidden, after):
    t = tile_of(width)
    rows = sum(p.shape[0] for p in parts)
    steps = width // t
    return pl.pallas_call(
        functools.partial(grads_kernel, len(parts), len(acts)),
        grid=(steps,),
        in_specs=[pl.BlockSpec((p.shape[0], t), lambda j: (0, j)) for p in parts]
        + [pl.BlockSpec((p.shape[0], t), lambda j: (0, j + steps)) for p in parts]
        + [whole(a.shape) for a in acts]
        + [UNREAD],
        out_specs=[
            pl.BlockSpec((t, hidden), lambda j: (j, 0)),
            pl.BlockSpec((t, hidden), lambda j: (j, 0)),
            pl.BlockSpec((hidden, t), lambda j: (0, j)),
        ],
        out_shape=[
            jax.ShapeDtypeStruct((width, hidden), BF),
            jax.ShapeDtypeStruct((width, hidden), BF),
            jax.ShapeDtypeStruct((hidden, width), BF),
        ],
        name="weight_grads",
        compiler_params=params(),
        cost_estimate=pl.CostEstimate(
            flops=6 * rows * width * hidden, bytes_accessed=6 * width * hidden, transcendentals=0
        ),
    )(*parts, *parts, *acts, after)


def merge_kernel(width, count, one_ref, two_ref, p_ref, *refs):
    parts = refs[:count]
    mixed, grad_tok, route = refs[1 + count :]
    tok = mixed.shape[0]
    one, two = one_ref[...], two_ref[...]
    eye = lax.broadcasted_iota(jnp.int32, (tok, tok), 0) == lax.broadcasted_iota(jnp.int32, (tok, tok), 1)
    p_one = jnp.sum(jnp.where(eye, p_ref[0:1, :], 0.0), axis=1, keepdims=True)
    p_two = jnp.sum(jnp.where(eye, p_ref[1:2, :], 0.0), axis=1, keepdims=True)
    out = gather_parts(parts, 0, width)
    mixed[...] = (p_one * dot(one, out, 0, 0) + p_two * dot(two, out, 0, 0)).astype(BF)
    dx = gather_parts(parts, width, 2 * width)
    both = one + two
    grad_tok[...] = dot(both, dx, 0, 0).astype(BF)
    inner = gather_parts(parts, 2 * width, 2 * width + R_LANES)
    route[0:1, :] = jnp.sum(dot(inner, one, 0, 0), axis=0, keepdims=True) / p_ref[0:1, :]
    route[1:2, :] = jnp.sum(dot(inner, two, 0, 0), axis=0, keepdims=True) / p_ref[1:2, :]


def merge(one, two, p, parts, tok, width, after):
    return pl.pallas_call(
        functools.partial(merge_kernel, width, len(parts)),
        in_specs=[whole(a.shape) for a in (one, two, p, *parts)] + [UNREAD],
        out_shape=[
            jax.ShapeDtypeStruct((tok, width), BF),
            jax.ShapeDtypeStruct((tok, width), BF),
            jax.ShapeDtypeStruct(p.shape, F32),
        ],
        name="merge_rows",
        compiler_params=params(),
        cost_estimate=pl.CostEstimate(flops=10**8, bytes_accessed=2 * 10**6, transcendentals=0),
    )(one, two, p, *parts, after)


def local(tokens, grad_out, expert_ids, route_weights, gate_weight, up_weight, down_weight):
    n = lax.axis_size("expert")
    n_dp = lax.axis_size("dp")
    assert gate_weight.shape[0] == 1
    weights = gate_weight[0], up_weight[0], down_weight[0]
    width, hidden = weights[0].shape
    tok = tokens.shape[0]
    top = expert_ids.shape[1]
    cap = max(2, 3 * tok * top // (2 * n))
    *sends, _, p, wg, wu, wd, one, two = send_rows(expert_ids.T, route_weights.T, tokens, grad_out, weights, n, cap)
    weights = wg, wu, wd
    plan = chained if chainable(n, n_dp) else plain
    parts, acts, returned, last = plan(sends, weights, cap)
    dg, du, dd = weight_grads(parts, acts, width, hidden, last)
    mixed, grad_tokens, route = merge(one, two, p, returned, tok, width, last)
    return (mixed, grad_tokens, route.T, dg[None], du[None], dd[None])


def chainable(n, n_dp):
    return n == 8 and n_dp == 4


def plain(sends, weights, cap):
    n = len(sends)
    order = jnp.arange(n) ^ lax.axis_index("expert")
    rows = jnp.stack(sends)[order]
    rows = lax.all_to_all(rows, "expert", split_axis=0, concat_axis=0, tiled=True)
    rows = rows.reshape(n * cap, -1)
    total = lax.psum(forward([rows], weights, rows), "dp")
    act, out = backward(total, total, None, 1, weights, (rows,))
    back = lax.all_to_all(out.reshape(n, cap, -1), "expert", split_axis=0, concat_axis=0, tiled=True)
    return [rows], [act], [back[order].reshape(n * cap, -1)], act


CHUNKS = {"O": (0, 1), "P": (2, 4), "D": (6, 7), "Q": (3, 5)}
SCRIPT = (
    ("send", "O"),
    ("send", "P"),
    ("fwd", "O"),
    ("fwd", "P"),
    ("send", "D"),
    ("one", "O"),
    ("send", "Q"),
    ("fwd", "D"),
    ("one", "P"),
    ("two", "O"),
    ("fwd", "Q"),
    ("one", "D"),
    ("two", "P"),
    ("bwd", "O"),
    ("one", "Q"),
    ("two", "D"),
    ("bwd", "P"),
    ("two", "Q"),
    ("bwd", "D"),
    ("bwd", "Q", "O"),
)


def chained(sends, weights, cap):
    n = len(sends)
    half = lax.axis_size("dp") // 2

    def is_end():
        z = lax.axis_index("dp")
        return jnp.logical_and(z != half - 1, z != half)

    def swap(array, x):
        return lax.ppermute(array, "expert", [(i, i ^ x) for i in range(n)]) if x else array

    def along(array, op):
        pairs = {"fwd": [(0, 1), (3, 2)], "one": [(1, 2), (2, 1)], "two": [(1, 0), (2, 3)]}[op]
        return array, lax.ppermute(array, "dp", pairs)

    last = sends[0]
    rows, flow, acts, back = {0: sends[0]}, {}, {}, {}
    for op, name, *behind in SCRIPT:
        chunk = CHUNKS[name]
        if op == "send":
            fresh = [sends[x] for x in chunk]
            if last is not sends[0]:
                fresh = hold(fresh, last)
                last = fresh[0]
            for x, array in zip(chunk, fresh):
                rows[x] = swap(array, x)
            continue
        if op == "fwd":
            last = forward([rows[x] for x in chunk], weights, last)
        elif op in ("one", "two"):
            last = add_rows(*flow[name], last)
        else:
            after = [back[x] for other in behind for x in CHUNKS[other]]
            last, *outs = backward(*flow[name], is_end, len(chunk), weights, (last, *after))
        if op == "bwd":
            acts[name] = last
            for x, out in zip(chunk, outs):
                back[x] = swap(out, x)
        else:
            flow[name] = along(last, op)
    parts = [rows[x] for chunk in CHUNKS.values() for x in chunk]
    return parts, [acts[name] for name in CHUNKS], [back[x] for x in range(n)], last


def solution(mesh):
    placed = (
        P("expert", "dp"),
        P("expert", "dp"),
        P("expert", None),
        P("expert", None),
        P("expert", "dp", None),
        P("expert", "dp", None),
        P("expert", None, "dp"),
    )
    return jax.shard_map(
        local,
        mesh=mesh,
        in_specs=placed,
        out_specs=(
            P("expert", "dp"),
            P("expert", "dp"),
            P("expert", None),
            P("expert", "dp", None),
            P("expert", "dp", None),
            P("expert", None, "dp"),
        ),
        check_vma=False,
    )
```
